8 devices in a mesh: data: 1 (over z), pp: 2 (over y), ep: 4 (over x, core).
Axes of the slice: x: 2, y: 2, z: 1, core: 2. Of those that a mesh axis runs over, the one named last changes fastest.
Arguments:
- o: bfloat16 [2, 1, 384, 32, 7168], P('pp', 'data', 'ep')
- idx: int32 [2, 1, 4, 256, 8], P('pp', 'data')
- slot: int32 [2, 1, 4, 256, 8], P('pp', 'data')
- gate: float32 [2, 1, 4, 256, 8], P('pp', 'data')
- h: bfloat16 [2, 1, 4, 256, 7168], P('pp', 'data', 'ep')
- norm_w: float32 [2, 7168], P('pp')
- wq: bfloat16 [2, 7168, 8192], P('pp')
- wk: bfloat16 [2, 7168, 8192], P('pp')
- wv: bfloat16 [2, 7168, 8192], P('pp')
- wo: bfloat16 [2, 8192, 7168], P('pp')
Outputs:
- output: bfloat16 [2, 1, 4, 256, 7168], P('pp', 'data', 'ep')
All inputs are finite; a program needn't handle non-finite values.
Results may differ from the reference program's by a relative error of at most 0.0106752.
Values are sent between devices in bfloat16 or wider.
A program may use at most 2 GiB of HBM per device.

```python
import jax
import jax.numpy as jnp
from jax import lax

PP = 2
EP = 4
M = 1
SEQ_DEV = 1
L = 256
D = 7168
E = 384
K = 8
R = 4
HEADS = 64
HEAD = 128

B = EP * SEQ_DEV
ELOC = E // EP
CAPD = 8 * ((3 * K * SEQ_DEV * L + 16 * E - 1) // (16 * E))
C = EP * CAPD
HD = HEADS * HEAD
EPS = 1e-6
SCALE = HEAD ** -0.5
WD = D ** -0.5
WH = HD ** -0.5


def route(key, dev, dev_bias, exp_bias):
    k1, k2, k3 = jax.random.split(key, 3)
    td = SEQ_DEV * L
    ds = jax.random.randint(k1, (td, EP), 0, 1 << 16) + dev_bias[None, :]
    chosen = jnp.argsort(-ds, axis=1)[:, :R]
    owner = jnp.arange(E) // ELOC
    allowed = jnp.any(owner[None, None, :] == chosen[:, :, None], axis=1)
    es = jax.random.randint(k2, (td, E), 0, 1 << 16) + exp_bias[None, :]
    es = jnp.where(allowed, es, -(1 << 30))
    ix = jnp.argsort(-es, axis=1)[:, :K].astype(jnp.int32)
    hot = (ix.reshape(td * K)[:, None] == jnp.arange(E)[None, :]).astype(jnp.int32)
    rank = jnp.sum(jnp.cumsum(hot, axis=0) * hot, axis=1) - 1
    sl = jnp.where(rank < CAPD, dev * CAPD + rank, -1).reshape(td, K).astype(jnp.int32)
    gg = 2.0 * jax.nn.softmax(1.5 * jax.random.normal(k3, (td, K), jnp.float32), axis=-1)
    return ix, sl, gg


def _route_spread(key, dev, dev_bias, exp_bias):
    lo = (K + ELOC - 1) // ELOC
    k1, k2, k3, k4, k5 = jax.random.split(key, 5)
    td = SEQ_DEV * L
    ds = jax.random.randint(k1, (td, EP), 0, 1 << 16) + dev_bias[None, :]
    rank_d = jnp.argsort(jnp.argsort(-ds, axis=1), axis=1)
    nd = jax.random.randint(k2, (td, 1), lo, R + 1)
    allowed = (rank_d < nd)[:, jnp.arange(E) // ELOC]
    es = jax.random.randint(k3, (td, E), 0, 1 << 16) + exp_bias[None, :]
    es = jnp.where(allowed, es, -(1 << 30))
    ix = jnp.argsort(-es, axis=1)[:, :K].astype(jnp.int32)
    hot = (ix.reshape(td * K)[:, None] == jnp.arange(E)[None, :]).astype(jnp.int32)
    rank = jnp.sum(jnp.cumsum(hot, axis=0) * hot, axis=1) - 1
    perm = jnp.argsort(jax.random.randint(k4, (E, CAPD), 0, 1 << 20), axis=1)
    pos = perm[ix.reshape(td * K), jnp.minimum(rank, CAPD - 1)]
    sl = jnp.where(rank < CAPD, dev * CAPD + pos, -1).reshape(td, K).astype(jnp.int32)
    gg = 2.0 * jax.nn.softmax(1.5 * jax.random.normal(k5, (td, K), jnp.float32), axis=-1)
    return ix, sl, gg


def setup_inputs(seed: int = 0, part: int = 0) -> dict:
    key = jax.random.fold_in(jax.random.key(seed), part)
    ks = jax.random.split(key, 8)
    kr = jax.random.split(jax.random.fold_in(key, 7), 3)
    dev_bias = jax.random.randint(kr[0], (EP,), 0, 1 << 15)
    exp_bias = jax.random.randint(kr[1], (E,), 0, 1 << 16)
    mu = jax.random.normal(ks[2], (PP, E, D), jnp.float32)
    sc = jax.random.uniform(ks[3], (PP, E), jnp.float32, 0.4, 1.6)

    def one_o(i):
        p = i // M
        nz = jax.random.normal(jax.random.fold_in(ks[4], i), (E, C, D), jnp.float32)
        return (sc[p][:, None, None] * (mu[p][:, None, :] + 0.5 * nz)).astype(jnp.bfloat16)

    o = lax.map(one_o, jnp.arange(PP * M)).reshape(PP, M, E, C, D)

    def one_r(i):
        return _route_spread(jax.random.fold_in(kr[2], i), i % EP, dev_bias, exp_bias)

    ix, sl, gg = lax.map(one_r, jnp.arange(PP * M * EP))
    cm = jax.random.normal(ks[6], (PP, M, B, 1, D), jnp.float32)
    nz = jax.random.normal(ks[7], (PP, M, B, L, D), jnp.float32)
    h = (0.6 * cm + 0.8 * nz).astype(jnp.bfloat16)
    kw = jax.random.split(jax.random.key(seed + 1), 5)
    norm_w = jax.random.uniform(kw[0], (PP, D), jnp.float32, 0.5, 1.5)
    wq = (1.4 * WD * jax.random.normal(kw[1], (PP, D, HD), jnp.float32)).astype(jnp.bfloat16)
    wk = (1.4 * WD * jax.random.normal(kw[2], (PP, D, HD), jnp.float32)).astype(jnp.bfloat16)
    wv = (WD * jax.random.normal(kw[3], (PP, D, HD), jnp.float32)).astype(jnp.bfloat16)
    wo = (WH * jax.random.normal(kw[4], (PP, HD, D), jnp.float32)).astype(jnp.bfloat16)
    return {'o': o, 'idx': ix.reshape(PP, M, B, L, K), 'slot': sl.reshape(PP, M, B, L, K), 'gate': gg.reshape(PP, M, B, L, K), 'h': h, 'norm_w': norm_w, 'wq': wq, 'wk': wk, 'wv': wv, 'wo': wo}


def _combine(o, ix, sl, gg, h):
    valid = sl >= 0
    rows = o.reshape(E * C, D)[jnp.where(valid, ix * C + sl, 0)].astype(jnp.float32)
    gw = jnp.where(valid, gg, 0.0)
    y = h.astype(jnp.float32) + jnp.sum(gw[..., None] * rows, axis=2)
    return y.astype(jnp.bfloat16)


def _attend(y, nw, wq, wk, wv, wo):
    yf = y.astype(jnp.float32)
    x = yf * lax.rsqrt(jnp.mean(yf * yf, axis=-1, keepdims=True) + EPS) * nw
    xb = x.astype(jnp.bfloat16).reshape(B * L, D)
    q = jnp.dot(xb, wq, preferred_element_type=jnp.float32).astype(jnp.bfloat16).reshape(B, L, HEADS, HEAD)
    kt = jnp.dot(xb, wk, preferred_element_type=jnp.float32).astype(jnp.bfloat16).reshape(B, L, HEADS, HEAD)
    vt = jnp.dot(xb, wv, preferred_element_type=jnp.float32).astype(jnp.bfloat16).reshape(B, L, HEADS, HEAD)
    causal = jnp.arange(L)[:, None] >= jnp.arange(L)[None, :]

    def one(a):
        s = jnp.einsum('qhd,khd->hqk', a[0].astype(jnp.float32), a[1].astype(jnp.float32)) * SCALE
        pr = jax.nn.softmax(jnp.where(causal[None], s, -1e30), axis=-1).astype(jnp.bfloat16)
        return jnp.einsum('hqk,khd->qhd', pr.astype(jnp.float32), a[2].astype(jnp.float32)).astype(jnp.bfloat16)

    att = lax.map(one, (q, kt, vt)).reshape(B * L, HD)
    out = jnp.dot(att, wo, preferred_element_type=jnp.float32).astype(jnp.bfloat16).reshape(B, L, D)
    return (yf + out.astype(jnp.float32)).astype(jnp.bfloat16)


def reference(o, idx, slot, gate, h, norm_w, wq, wk, wv, wo):
    y = lax.map(lambda a: _combine(a[0], a[1], a[2], a[3], a[4]), (o.reshape(PP * M, E, C, D), idx.reshape(PP * M, B, L, K), slot.reshape(PP * M, B, L, K), gate.reshape(PP * M, B, L, K), h.reshape(PP * M, B, L, D)))
    yin = jnp.roll(y.reshape(PP, M, B, L, D), 1, axis=0).reshape(PP * M, B, L, D)
    stage = jnp.arange(PP * M) // M
    z = lax.map(lambda a: _attend(a[0], norm_w[a[1]], wq[a[1]], wk[a[1]], wv[a[1]], wo[a[1]]), (yin, stage))
    return z.reshape(PP, M, B, L, D)
```

```python
import functools

import jax
import jax.numpy as jnp
from jax import lax
from jax.experimental import pallas as pl
from jax.experimental.pallas import tpu as pltpu
from jax.sharding import PartitionSpec as P

HEAD = 128
EPS = 1e-6
SCALE = HEAD ** -0.5
MESH = pl.DeviceIdType.MESH
F32 = jnp.float32
BF16 = jnp.bfloat16
CH = 512
NS = 4
WN = 2048
SHIFT = 2.0 ** -40


def kernel(n_ep, el, capd, idx_ref, slot_ref, gate_ref, nw_ref, o_hbm, h_hbm, wq_hbm, wk_hbm, wv_hbm, wo_hbm,
           z_hbm, send, base, xrecv, yin, ssq, rs_ref,
           s_d2r, r_d2r, s_d2o, r_d2o, s_x, r_x, s_y, r_y, s_w, s_o, s_h, s_z):
    p = lax.axis_index('pp')
    me = lax.axis_index('ep')
    mate = me + 1 - 2 * lax.rem(me, 2)
    xpeer = lax.rem(me + 2, n_ep)
    xmate = mate + 2 - 4 * (mate // 2)
    ydev = {'pp': 1 - p}
    xdev = {'ep': xpeer}
    mdev = {'ep': mate}
    nc = send.shape[0]
    ln = send.shape[1]
    ns = el * capd
    nh = wq_hbm.shape[1] // HEAD
    ng = nh * HEAD // CH
    d = wo_hbm.shape[1]
    wj = wq_hbm.shape[1] // WN
    hbms = (wq_hbm, wk_hbm, wv_hbm)

    barrier = pltpu.get_barrier_semaphore()
    for dev in (mdev, xdev, ydev):
        pl.semaphore_signal(barrier, inc=1, device_id=dev, device_id_type=MESH)
    pl.semaphore_wait(barrier, 3)

    dests = (xmate, mate, xpeer, me)

    def produce(gm, oslab, stage, hbuf):
        def ocopy(n, q):
            sl = lax.rem(n, 2)
            return pltpu.make_async_copy(
                o_hbm.at[:, dests[q], :, pl.ds(pl.multiple_of(n * CH, CH), CH)], oslab.at[sl, q], s_o.at[sl, q])

        hcopy = pltpu.make_async_copy(h_hbm, hbuf, s_h)
        hcopy.start()
        for q in range(4):
            ocopy(0, q).start()
        iota = lax.broadcasted_iota(jnp.int32, (ln, ns), 1)

        def build(q):
            j = dests[q]
            loc = idx_ref[j] - el * me
            sl = slot_ref[j]
            ok = (sl >= 0) & (loc >= 0) & (loc < el)
            flat = jnp.where(ok, loc * capd + sl - j * capd, -1)
            gt = gate_ref[j]
            a = jnp.zeros((ln, ns), F32)
            for k in range(flat.shape[1]):
                a = a + jnp.where(iota == flat[:, k:k + 1], gt[:, k:k + 1], 0.0)
            g1 = a.astype(BF16)
            a = a - g1.astype(F32)
            g2 = a.astype(BF16)
            a = a - g2.astype(F32)
            gm[q, 0:ln] = g1
            gm[q, ln:2 * ln] = g2
            gm[q, 2 * ln:3 * ln] = a.astype(BF16)

        for q in range(4):
            build(q)
        hcopy.wait()

        def rsend(n):
            return pltpu.make_async_remote_copy(stage.at[0, lax.rem(n, 2)], send.at[n], s_d2r.at[lax.rem(n, 2)], r_d2r.at[n],
                                                device_id=mdev, device_id_type=MESH)

        def osend(n):
            return pltpu.make_async_remote_copy(stage.at[1, lax.rem(n, 2)], base.at[n], s_d2o.at[lax.rem(n, 2)], r_d2o.at[n],
                                                device_id=mdev, device_id_type=MESH)

        def part(n, q):
            ocopy(n, q).wait()
            r = jnp.dot(gm[q], oslab[lax.rem(n, 2), q].reshape(ns, CH), preferred_element_type=F32)
            return r[0:ln] + r[ln:2 * ln] + r[2 * ln:3 * ln]

        def step(n, _):
            @pl.when(n + 1 < nc)
            def _():
                for q in range(4):
                    ocopy(n + 1, q).start()

            @pl.when(n >= 2)
            def _():
                rsend(n - 2).wait_send()
                osend(n - 2).wait_send()
            b = lax.rem(n, 2)
            stage[0, b] = part(n, 0)
            rsend(n).start()
            stage[1, b] = part(n, 1)
            osend(n).start()
            mine = part(n, 2)
            rsend(n).wait_recv()
            send[n] = send[n] + mine
            own = part(n, 3) + hbuf[:, pl.ds(pl.multiple_of(n * CH, CH), CH)].astype(F32)
            xsend(n).start()
            osend(n).wait_recv()
            base[n] = base[n] + own
            return 0

        lax.fori_loop(0, nc, step, 0)
        for n in (nc - 2, nc - 1):
            rsend(n).wait_send()
            osend(n).wait_send()

    def xsend(n):
        return pltpu.make_async_remote_copy(send.at[n], xrecv.at[n], s_x.at[n], r_x.at[n],
                                            device_id=xdev, device_id_type=MESH)

    pl.run_scoped(produce,
                  pltpu.VMEM((4, 3 * ln, ns), BF16),
                  pltpu.VMEM((2, 4, el, capd, CH), BF16),
                  pltpu.VMEM((2, 2, ln, CH), F32),
                  pltpu.VMEM((ln, d), BF16))

    def main(acc, wbuf, ystage):
        def wcopy(n, i):
            src = hbms[i // wj].at[pl.ds(pl.multiple_of(n * CH, CH), CH), pl.ds((i % wj) * WN, WN)]
            return pltpu.make_async_copy(src, wbuf.at[i % NS], s_w.at[i % NS])

        def ocopy(g, i):
            wd = min(WN, d - i * WN)
            src = wo_hbm.at[pl.ds(pl.multiple_of(g * CH, CH), CH), pl.ds(i * WN, wd)]
            return pltpu.make_async_copy(src, wbuf.at[i, :, 0:wd], s_w.at[i])

        def ysend(n):
            return pltpu.make_async_remote_copy(ystage.at[lax.rem(n, 2)], yin.at[n], s_y.at[lax.rem(n, 2)], r_y.at[n],
                                                device_id=ydev, device_id_type=MESH)

        for i in range(NS):
            wcopy(0, i).start()

        def zero(i, _):
            acc[i] = jnp.zeros(acc.shape[1:], F32)
            return 0
        lax.fori_loop(0, acc.shape[0], zero, 0)
        ssq[...] = jnp.zeros_like(ssq)

        def service(n):
            @pl.when(n >= 2)
            def _():
                ysend(n - 2).wait_send()
            xsend(n).wait_recv()
            ystage[lax.rem(n, 2)] = (base[n] + xrecv[n]).astype(BF16)
            ysend(n).start()

        service(0)
        nj = 3 * wj

        def chunk(n, _):
            @pl.when(n + 1 < nc)
            def _():
                service(n + 1)
            ysend(n).wait_recv()
            yf = yin[n].astype(F32)
            y2 = yf * yf
            ssq[...] += y2[:, 0:128] + y2[:, 128:256] + y2[:, 256:384] + y2[:, 384:512]
            xw = (yf * (nw_ref[n] * SHIFT)).astype(BF16)
            for i in range(nj):
                wcopy(n, i).wait()
                for b in range(WN // CH):
                    k = i * (WN // CH) + b
                    acc[k] += jnp.dot(xw, wbuf[i % NS, :, b * CH:(b + 1) * CH], preferred_element_type=F32)
                if i + NS < nj:
                    wcopy(n, i + NS).start()
                else:
                    ii = i + NS - nj

                    @pl.when(n + 1 < nc)
                    def _():
                        wcopy(n + 1, ii).start()

                    @pl.when(n + 1 == nc)
                    def _():
                        ocopy(0, ii).start()
            return 0

        lax.fori_loop(0, nc, chunk, 0)
        ysend(nc - 2).wait_send()
        ysend(nc - 1).wait_send()
        for n in range(nc):
            xsend(n).wait_send()

        def zero2(i, _):
            send[i] = jnp.zeros(send.shape[1:], F32)
            return 0
        lax.fori_loop(0, nc, zero2, 0)
        ms = jnp.sum(ssq[...], axis=1, keepdims=True) / d
        rs_ref[...] = jnp.broadcast_to(lax.rsqrt(ms + EPS) * (1.0 / SHIFT), rs_ref.shape)

        row = lax.broadcasted_iota(jnp.int32, (ln, ln), 0)
        col = lax.broadcasted_iota(jnp.int32, (ln, ln), 1)

        def group(g, _):
            rs = rs_ref[:, 0:1]
            q4 = (acc[g] * rs).astype(BF16)
            k4 = (acc[ng + g] * rs).astype(BF16)
            v4 = (acc[2 * ng + g] * rs).astype(BF16)
            outs = []
            for hh in range(CH // HEAD):
                c = slice(hh * HEAD, (hh + 1) * HEAD)
                s = lax.dot_general(q4[:, c], k4[:, c], (((1,), (1,)), ((), ())), preferred_element_type=F32) * SCALE
                s = jnp.where(row >= col, s, -1e30)
                e = jnp.exp(s - jnp.max(s, axis=1, keepdims=True))
                pr = (e * (1.0 / jnp.sum(e, axis=1, keepdims=True))).astype(BF16)
                outs.append(jnp.dot(pr, v4[:, c], preferred_element_type=F32).astype(BF16))
            a4 = jnp.concatenate(outs, axis=1)
            for i in range(NS):
                ocopy(g, i).wait()
                wd = min(WN, d - i * WN)
                for b in range(wd // CH):
                    k = i * (WN // CH) + b
                    send[k] += jnp.dot(a4, wbuf[i, :, b * CH:(b + 1) * CH], preferred_element_type=F32)

                @pl.when(g + 1 < ng)
                def _():
                    ocopy(g + 1, i).start()
            return 0

        lax.fori_loop(0, ng, group, 0)

        def zcopy(n):
            return pltpu.make_async_copy(yin.at[n], z_hbm.at[:, pl.ds(pl.multiple_of(n * CH, CH), CH)], s_z.at[n])

        def fin(n, _):
            yin[n] = (yin[n].astype(F32) + send[n].astype(BF16).astype(F32)).astype(BF16)
            zcopy(n).start()
            return 0
        lax.fori_loop(0, nc, fin, 0)

        def finw(n, _):
            zcopy(n).wait()
            return 0
        lax.fori_loop(0, nc, finw, 0)

    pl.run_scoped(main,
                  pltpu.VMEM((3 * ng, ln, CH), F32),
                  pltpu.VMEM((NS, CH, WN), BF16),
                  pltpu.VMEM((2, ln, CH), BF16))


def solution(mesh):
    n = mesh.shape['ep']
    sp_o = P('pp', 'data', 'ep', None, None)
    sp_r = P('pp', 'data', None, None, None)
    sp_1 = P('pp', None)
    sp_w = P('pp', None, None)

    def body(o, idx, slot, gate, h, norm_w, wq, wk, wv, wo):
        el, c, d = o.shape[2:]
        capd = c // n
        ln = h.shape[3]
        nc = d // CH
        ng = wq.shape[2] // CH
        sem = pltpu.SemaphoreType.DMA
        vm = pl.BlockSpec(memory_space=pltpu.VMEM)
        hb = pl.BlockSpec(memory_space=pltpu.HBM)
        z = pl.pallas_call(
            functools.partial(kernel, n, el, capd),
            out_shape=jax.ShapeDtypeStruct((ln, d), BF16),
            in_specs=[vm] * 4 + [hb] * 6,
            out_specs=hb,
            scratch_shapes=[
                pltpu.VMEM((nc, ln, CH), F32),
                pltpu.VMEM((nc, ln, CH), F32),
                pltpu.VMEM((nc, ln, CH), F32),
                pltpu.VMEM((nc, ln, CH), BF16),
                pltpu.VMEM((ln, 128), F32),
                pltpu.VMEM((ln, 128), F32),
                sem((2,)), sem((nc,)), sem((2,)), sem((nc,)), sem((nc,)), sem((nc,)), sem((2,)), sem((nc,)),
                sem((NS,)), sem((2, 4)), sem, sem((nc,)),
            ],
            compiler_params=pltpu.CompilerParams(collective_id=0, has_side_effects=True, vmem_limit_bytes=67043328),
        )(idx[0, 0], slot[0, 0], gate[0, 0], norm_w.reshape(nc, 1, CH), o.reshape(el, n, capd, d), h[0, 0, 0],
          wq[0], wk[0], wv[0], wo[0])
        return z.reshape(1, 1, 1, ln, d)

    return jax.shard_map(body, mesh=mesh, in_specs=(sp_o, sp_r, sp_r, sp_r, sp_o, sp_1, sp_w, sp_w, sp_w, sp_w), out_specs=sp_o, check_vma=False)
```

```python
import functools

import jax
import jax.numpy as jnp
from jax import lax
from jax.experimental import pallas as pl
from jax.experimental.pallas import tpu as pltpu
from jax.sharding import PartitionSpec as P

HEAD = 128
EPS = 1e-6
SCALE = HEAD ** -0.5
SCALE2 = SCALE * 1.4426950408889634
MASKED = -1e30 / SCALE
QB = 128
MESH = pl.DeviceIdType.MESH
F32 = jnp.float32
BF16 = jnp.bfloat16
CH = 512
NS = 4
WN = 2048
SHIFT = 2.0 ** -40
HEADS_AT = ((0, 1, 2, 3), (), (), ())


def kernel(n_ep, el, capd, idx_ref, slot_ref, gate_ref, nw_ref, o_hbm, h_hbm, wq_hbm, wk_hbm, wv_hbm, wo_hbm,
           z_hbm, send, base, xrecv, yin, ssq, rs_ref,
           s_d2r, r_d2r, s_d2o, r_d2o, s_x, r_x, s_y, r_y, s_w, s_o, s_h):
    p = lax.axis_index('pp')
    me = lax.axis_index('ep')
    mate = me + 1 - 2 * lax.rem(me, 2)
    xpeer = lax.rem(me + 2, n_ep)
    xmate = mate + 2 - 4 * (mate // 2)
    ydev = {'pp': 1 - p}
    xdev = {'ep': xpeer}
    mdev = {'ep': mate}
    nc = send.shape[0]
    ln = send.shape[1]
    ns = el * capd
    nh = wq_hbm.shape[1] // HEAD
    ng = nh * HEAD // CH
    d = wo_hbm.shape[1]
    wj = wq_hbm.shape[1] // WN
    hbms = (wq_hbm, wk_hbm, wv_hbm)

    barrier = pltpu.get_barrier_semaphore()
    for dev in (mdev, xdev, ydev):
        pl.semaphore_signal(barrier, inc=1, device_id=dev, device_id_type=MESH)

    dests = (xmate, mate, xpeer, me)

    def produce(gm, oslab, stage, hbuf):
        def ocopy(n, q):
            sl = lax.rem(n, 2)
            return pltpu.make_async_copy(
                o_hbm.at[:, dests[q], :, pl.ds(pl.multiple_of(n * CH, CH), CH)], oslab.at[sl, q], s_o.at[sl, q])

        hcopy = pltpu.make_async_copy(h_hbm, hbuf, s_h)
        hcopy.start()
        for q in range(4):
            ocopy(0, q).start()
        iota = lax.broadcasted_iota(jnp.int32, (ln, ns), 1)

        def build(q):
            j = dests[q]
            loc = idx_ref[j] - el * me
            sl = slot_ref[j]
            ok = (sl >= 0) & (loc >= 0) & (loc < el)
            kk = sl.shape[0]
            pad = jnp.zeros((128 - kk, ln), F32)
            flat = jnp.where(ok, loc * capd + sl - j * capd, -1).astype(F32)
            flat = jnp.concatenate([flat, pad], axis=0).T[:, 0:kk].astype(jnp.int32)
            gt = jnp.concatenate([gate_ref[j], pad], axis=0).T[:, 0:kk]
            a = jnp.zeros((ln, ns), F32)
            for k in range(kk):
                a = a + jnp.where(iota == flat[:, k:k + 1], gt[:, k:k + 1], 0.0)
            g1 = a.astype(BF16)
            a = a - g1.astype(F32)
            g2 = a.astype(BF16)
            a = a - g2.astype(F32)
            gm[q, 0:ln] = g1
            gm[q, ln:2 * ln] = g2
            gm[q, 2 * ln:3 * ln] = a.astype(BF16)


        def rsend(n):
            return pltpu.make_async_remote_copy(stage.at[0, lax.rem(n, 2)], send.at[n], s_d2r.at[lax.rem(n, 2)], r_d2r.at[n],
                                                device_id=mdev, device_id_type=MESH)

        def osend(n):
            return pltpu.make_async_remote_copy(stage.at[1, lax.rem(n, 2)], base.at[n], s_d2o.at[lax.rem(n, 2)], r_d2o.at[n],
                                                device_id=mdev, device_id_type=MESH)

        def part(n, q):
            ocopy(n, q).wait()
            r = jnp.dot(gm[q], oslab[lax.rem(n, 2), q].reshape(ns, CH), preferred_element_type=F32)
            return r[0:ln] + r[ln:2 * ln] + r[2 * ln:3 * ln]

        def fetch(n):
            @pl.when(n + 1 < nc)
            def _():
                for q in range(4):
                    ocopy(n + 1, q).start()

        def away(n):
            stage[0, lax.rem(n, 2)] = part(n, 0)
            rsend(n).start()

        def away2(n):
            mine = part(n, 2)
            rsend(n).wait_recv()
            send[n] = send[n] + mine

        def near(n):
            stage[1, lax.rem(n, 2)] = part(n, 1)
            osend(n).start()

        def near2(n):
            own = part(n, 3) + hbuf[:, pl.ds(pl.multiple_of(n * CH, CH), CH)].astype(F32)
            osend(n).wait_recv()
            base[n] = base[n] + own

        fetch(0)
        build(0)
        pl.semaphore_wait(barrier, 3)
        away(0)
        build(2)
        away2(0)
        xsend(0).start()
        build(1)
        near(0)
        build(3)
        hcopy.wait()
        near2(0)

        def step(n, _):
            fetch(n)

            @pl.when(n >= 2)
            def _():
                rsend(n - 2).wait_send()
                osend(n - 2).wait_send()
            away(n)
            near(n)
            away2(n)
            own = part(n, 3) + hbuf[:, pl.ds(pl.multiple_of(n * CH, CH), CH)].astype(F32)
            xsend(n).start()
            osend(n).wait_recv()
            base[n] = base[n] + own
            return 0

        lax.fori_loop(1, nc, step, 0)
        for n in (nc - 2, nc - 1):
            rsend(n).wait_send()
            osend(n).wait_send()

    def xsend(n):
        return pltpu.make_async_remote_copy(send.at[n], xrecv.at[n], s_x.at[n], r_x.at[n],
                                            device_id=xdev, device_id_type=MESH)

    pl.run_scoped(produce,
                  pltpu.VMEM((4, 3 * ln, ns), BF16),
                  pltpu.VMEM((2, 4, el, capd, CH), BF16),
                  pltpu.VMEM((2, 2, ln, CH), F32),
                  pltpu.VMEM((ln, d), BF16))

    def main(acc, wbuf, ystage, abuf0, abuf1):
        def wcopy(n, i):
            src = hbms[i // wj].at[pl.ds(pl.multiple_of(n * CH, CH), CH), pl.ds((i % wj) * WN, WN)]
            return pltpu.make_async_copy(src, wbuf.at[i % NS], s_w.at[i % NS])

        def ocopy(g, i):
            wd = min(WN, d - i * WN)
            src = wo_hbm.at[pl.ds(pl.multiple_of(g * CH, CH), CH), pl.ds(i * WN, wd)]
            return pltpu.make_async_copy(src, wbuf.at[i, :, 0:wd], s_w.at[i])

        def ysend(n):
            return pltpu.make_async_remote_copy(ystage.at[lax.rem(n, 2)], yin.at[n], s_y.at[lax.rem(n, 2)], r_y.at[n],
                                                device_id=ydev, device_id_type=MESH)

        for i in range(NS):
            wcopy(0, i).start()

        def zero(i, _):
            acc[i] = jnp.zeros(acc.shape[1:], F32)
            return 0
        lax.fori_loop(0, acc.shape[0], zero, 0)
        ssq[...] = jnp.zeros_like(ssq)

        def service(n):
            @pl.when(n >= 2)
            def _():
                ysend(n - 2).wait_send()
            xsend(n).wait_recv()
            ystage[lax.rem(n, 2)] = (base[n] + xrecv[n]).astype(BF16)
            ysend(n).start()

        def clear(n):
            xsend(n).wait_send()
            send[n] = jnp.zeros(send.shape[1:], F32)

        service(0)
        nj = 3 * wj

        def chunk(n, _):
            @pl.when(n + 1 < nc)
            def _():
                service(n + 1)
            @pl.when(n >= 2)
            def _():
                clear(n - 2)
            ysend(n).wait_recv()
            yf = yin[n].astype(F32)
            y2 = yf * yf
            ssq[...] += y2[:, 0:128] + y2[:, 128:256] + y2[:, 256:384] + y2[:, 384:512]
            xw = (yf * (nw_ref[n] * SHIFT)).astype(BF16)
            for i in range(nj):
                wcopy(n, i).wait()
                for b in range(WN // CH):
                    k = i * (WN // CH) + b
                    acc[k] += jnp.dot(xw, wbuf[i % NS, :, b * CH:(b + 1) * CH], preferred_element_type=F32)
                if i + NS < nj:
                    wcopy(n, i + NS).start()
                else:
                    ii = i + NS - nj

                    @pl.when(n + 1 < nc)
                    def _():
                        wcopy(n + 1, ii).start()

                    @pl.when(n + 1 == nc)
                    def _():
                        ocopy(0, ii).start()
            return 0

        lax.fori_loop(0, nc, chunk, 0)
        ysend(nc - 2).wait_send()
        ysend(nc - 1).wait_send()
        for n in (nc - 2, nc - 1):
            clear(n)
        ms = jnp.sum(ssq[...], axis=1, keepdims=True) / d
        rs_ref[...] = jnp.broadcast_to(lax.rsqrt(ms + EPS) * (1.0 / SHIFT), rs_ref.shape)

        tri = lax.broadcasted_iota(jnp.int32, (QB, QB), 0) >= lax.broadcasted_iota(jnp.int32, (QB, QB), 1)

        def qkv(g, hh):
            rs = rs_ref[:, 0:1]
            c = slice(hh * HEAD, (hh + 1) * HEAD)
            return [(acc[m * ng + g, :, c] * rs).astype(BF16) for m in range(3)]

        def heads(g, hhs, dst):
            tiles = [(hh, r) for hh in hhs for r in range(ln // QB)]
            qk = {hh: qkv(g, hh) for hh in hhs}
            sc = []
            for hh, r in tiles:
                lo, hi = r * QB, (r + 1) * QB
                q, k, _ = qk[hh]
                s = lax.dot_general(q[lo:hi], k[0:hi], (((1,), (1,)), ((), ())), preferred_element_type=F32)
                t = jnp.where(tri, s[:, lo:hi], MASKED)
                sc.append(t if r == 0 else jnp.concatenate([s[:, 0:lo], t], axis=1))
            mx = [jnp.max(s, axis=1, keepdims=True) for s in sc]
            ex = [jnp.exp2((s - m) * SCALE2) for s, m in zip(sc, mx)]
            rc = [1.0 / jnp.sum(e, axis=1, keepdims=True) for e in ex]
            pr = [(e * c).astype(BF16) for e, c in zip(ex, rc)]
            for (hh, r), w in zip(tiles, pr):
                lo, hi = r * QB, (r + 1) * QB
                dst[lo:hi, hh * HEAD:(hh + 1) * HEAD] = jnp.dot(w, qk[hh][2][0:hi], preferred_element_type=F32).astype(BF16)

        heads(0, range(CH // HEAD), abuf0)

        def group(g, src, dst):
            g1 = jnp.minimum(g + 1, ng - 1)
            for i in range(NS):
                ocopy(g, i).wait()
                wd = min(WN, d - i * WN)
                for b in range(wd // CH):
                    k = i * (WN // CH) + b
                    send[k] += jnp.dot(src[...], wbuf[i, :, b * CH:(b + 1) * CH], preferred_element_type=F32)
                if HEADS_AT[i]:
                    heads(g1, HEADS_AT[i], dst)

                @pl.when(g + 1 < ng)
                def _():
                    ocopy(g + 1, i).start()

        def pair(gg, _):
            group(2 * gg, abuf0, abuf1)
            group(2 * gg + 1, abuf1, abuf0)
            return 0

        lax.fori_loop(0, ng // 2, pair, 0)

        def fin(n, _):
            z_hbm[:, pl.ds(pl.multiple_of(n * CH, CH), CH)] = (
                yin[n].astype(F32) + send[n].astype(BF16).astype(F32)).astype(BF16)
            return 0
        lax.fori_loop(0, nc, fin, 0)

    pl.run_scoped(main,
                  pltpu.VMEM((3 * ng, ln, CH), F32),
                  pltpu.VMEM((NS, CH, WN), BF16),
                  pltpu.VMEM((2, ln, CH), BF16),
                  pltpu.VMEM((ln, CH), BF16),
                  pltpu.VMEM((ln, CH), BF16))


def solution(mesh):
    n = mesh.shape['ep']
    sp_o = P('pp', 'data', 'ep', None, None)
    sp_r = P('pp', 'data', None, None, None)
    sp_1 = P('pp', None)
    sp_w = P('pp', None, None)

    def body(o, idx, slot, gate, h, norm_w, wq, wk, wv, wo):
        el, c, d = o.shape[2:]
        capd = c // n
        ln = h.shape[3]
        nc = d // CH
        ng = wq.shape[2] // CH
        sem = pltpu.SemaphoreType.DMA
        vm = pl.BlockSpec(memory_space=pltpu.VMEM)
        hb = pl.BlockSpec(memory_space=pltpu.HBM)
        z = pl.pallas_call(
            functools.partial(kernel, n, el, capd),
            out_shape=pltpu.VMEM((ln, d), BF16),
            in_specs=[vm] * 4 + [hb] * 6,
            out_specs=vm,
            scratch_shapes=[
                pltpu.VMEM((nc, ln, CH), F32),
                pltpu.VMEM((nc, ln, CH), F32),
                pltpu.VMEM((nc, ln, CH), F32),
                pltpu.VMEM((nc, ln, CH), BF16),
                pltpu.VMEM((ln, 128), F32),
                pltpu.VMEM((ln, 128), F32),
                sem((2,)), sem((nc,)), sem((2,)), sem((nc,)), sem((nc,)), sem((nc,)), sem((2,)), sem((nc,)),
                sem((NS,)), sem((2, 4)), sem,
            ],
            compiler_params=pltpu.CompilerParams(collective_id=0, has_side_effects=True, vmem_limit_bytes=63000000),
        )(jnp.swapaxes(idx[0, 0], 1, 2), jnp.swapaxes(slot[0, 0], 1, 2), jnp.swapaxes(gate[0, 0], 1, 2), norm_w.reshape(nc, 1, CH), o.reshape(el, n, capd, d), h[0, 0, 0],
          wq[0], wk[0], wv[0], wo[0])
        return z.reshape(1, 1, 1, ln, d)

    return jax.shard_map(body, mesh=mesh, in_specs=(sp_o, sp_r, sp_r, sp_r, sp_o, sp_1, sp_w, sp_w, sp_w, sp_w), out_specs=sp_o, check_vma=False)
```

```python
import functools

import jax
import jax.numpy as jnp
from jax import lax
from jax.experimental import pallas as pl
from jax.experimental.pallas import tpu as pltpu
from jax.sharding import PartitionSpec as P

HEAD = 128
EPS = 1e-6
SCALE = HEAD ** -0.5
SCALE2 = SCALE * 1.4426950408889634
MASKED = -1e30 / SCALE
QB = 128
MESH = pl.DeviceIdType.MESH
F32 = jnp.float32
BF16 = jnp.bfloat16
CH = 512
NS = 4
WN = 2048
SHIFT = 2.0 ** -40
EARLY = (6, 10)
LATE = 5
HEADS_AT = ((0, 1, 2, 3), (), (), ())


def kernel(n_ep, el, capd, idx_ref, slot_ref, gate_ref, nw_ref, o_hbm, h_hbm, wq_hbm, wk_hbm, wv_hbm, wo_hbm,
           z_hbm, send, base, xrecv, yin, ssq, rs_ref, ystage,
           s_d2r, r_d2r, s_d2o, r_d2o, s_x, r_x, s_y, r_y, s_w, s_o, s_h):
    p = lax.axis_index('pp')
    me = lax.axis_index('ep')
    mate = me + 1 - 2 * lax.rem(me, 2)
    xpeer = lax.rem(me + 2, n_ep)
    xmate = mate + 2 - 4 * (mate // 2)
    ydev = {'pp': 1 - p}
    xdev = {'ep': xpeer}
    mdev = {'ep': mate}
    nc = send.shape[0]
    ln = send.shape[1]
    ns = el * capd
    nh = wq_hbm.shape[1] // HEAD
    ng = nh * HEAD // CH
    d = wo_hbm.shape[1]
    wj = wq_hbm.shape[1] // WN
    hbms = (wq_hbm, wk_hbm, wv_hbm)

    barrier = pltpu.get_barrier_semaphore()
    for dev in (mdev, xdev, ydev):
        pl.semaphore_signal(barrier, inc=1, device_id=dev, device_id_type=MESH)

    dests = (xmate, mate, xpeer, me)

    def xsend(n):
        return pltpu.make_async_remote_copy(send.at[n], xrecv.at[n], s_x.at[n], r_x.at[n],
                                            device_id=xdev, device_id_type=MESH)

    def ysend(n):
        return pltpu.make_async_remote_copy(ystage.at[lax.rem(n, 2)], yin.at[n], s_y.at[lax.rem(n, 2)], r_y.at[n],
                                            device_id=ydev, device_id_type=MESH)

    hr = ln // 2

    def xlast(f):
        c = pl.ds(f * hr, hr)
        return pltpu.make_async_remote_copy(send.at[nc - 1, c], xrecv.at[nc - 1, c], s_x.at[nc - 1 + f], r_x.at[nc - 1 + f],
                                            device_id=xdev, device_id_type=MESH)

    def ylast(f):
        c = pl.ds(f * hr, hr)
        b = (nc - 1) % 2
        return pltpu.make_async_remote_copy(ystage.at[b, c], yin.at[nc - 1, c], s_y.at[b + f], r_y.at[nc - 1 + f],
                                            device_id=ydev, device_id_type=MESH)

    def service_last(f):
        if f == 0:
            ysend(nc - 3).wait_send()
        xlast(f).wait_recv()
        c = slice(f * hr, (f + 1) * hr)
        ystage[(nc - 1) % 2, c] = (base[nc - 1, c] + xrecv[nc - 1, c]).astype(BF16)
        ylast(f).start()

    def service(n):
        @pl.when(n >= 2)
        def _():
            ysend(n - 2).wait_send()
        xsend(n).wait_recv()
        ystage[lax.rem(n, 2)] = (base[n] + xrecv[n]).astype(BF16)
        ysend(n).start()

    def produce(gm, oslab, stage, hbuf):
        def ocopy(n, q):
            sl = lax.rem(n, 2)
            return pltpu.make_async_copy(
                o_hbm.at[:, dests[q], :, pl.ds(pl.multiple_of(n * CH, CH), CH)], oslab.at[sl, q], s_o.at[sl, q])

        hcopy = pltpu.make_async_copy(h_hbm, hbuf, s_h)
        hcopy.start()
        for q in range(4):
            ocopy(0, q).start()
        iota = lax.broadcasted_iota(jnp.int32, (ln, ns), 1)

        def build(q):
            j = dests[q]
            loc = idx_ref[j] - el * me
            sl = slot_ref[j]
            ok = (sl >= 0) & (loc >= 0) & (loc < el)
            kk = sl.shape[0]
            pad = jnp.zeros((128 - kk, ln), F32)
            flat = jnp.where(ok, loc * capd + sl - j * capd, -1).astype(F32)
            flat = jnp.concatenate([flat, pad], axis=0).T[:, 0:kk].astype(jnp.int32)
            gt = jnp.concatenate([gate_ref[j], pad], axis=0).T[:, 0:kk]
            a = jnp.zeros((ln, ns), F32)
            for k in range(kk):
                a = a + jnp.where(iota == flat[:, k:k + 1], gt[:, k:k + 1], 0.0)
            g1 = a.astype(BF16)
            a = a - g1.astype(F32)
            g2 = a.astype(BF16)
            a = a - g2.astype(F32)
            gm[q, 0:ln] = g1
            gm[q, ln:2 * ln] = g2
            gm[q, 2 * ln:3 * ln] = a.astype(BF16)


        def rsend(n):
            return pltpu.make_async_remote_copy(stage.at[0, lax.rem(n, 2)], send.at[n], s_d2r.at[lax.rem(n, 2)], r_d2r.at[n],
                                                device_id=mdev, device_id_type=MESH)

        def osend(n):
            return pltpu.make_async_remote_copy(stage.at[1, lax.rem(n, 2)], base.at[n], s_d2o.at[lax.rem(n, 2)], r_d2o.at[n],
                                                device_id=mdev, device_id_type=MESH)

        def part(n, q):
            ocopy(n, q).wait()
            r = jnp.dot(gm[q], oslab[lax.rem(n, 2), q].reshape(ns, CH), preferred_element_type=F32)
            return r[0:ln] + r[ln:2 * ln] + r[2 * ln:3 * ln]

        def fetch(n):
            @pl.when(n + 1 < nc)
            def _():
                for q in range(4):
                    ocopy(n + 1, q).start()

        def away(n):
            stage[0, lax.rem(n, 2)] = part(n, 0)
            rsend(n).start()

        def away2(n):
            mine = part(n, 2)
            rsend(n).wait_recv()
            send[n] = send[n] + mine

        def near(n):
            stage[1, lax.rem(n, 2)] = part(n, 1)
            osend(n).start()

        def near2(n):
            own = part(n, 3) + hbuf[:, pl.ds(pl.multiple_of(n * CH, CH), CH)].astype(F32)
            osend(n).wait_recv()
            base[n] = base[n] + own

        fetch(0)
        build(0)
        pl.semaphore_wait(barrier, 3)
        away(0)
        build(2)
        away2(0)
        xsend(0).start()
        build(1)
        near(0)
        build(3)
        hcopy.wait()
        near2(0)

        def step(n, _):
            fetch(n)

            @pl.when(n >= 2)
            def _():
                rsend(n - 2).wait_send()
                osend(n - 2).wait_send()
            away(n)
            near(n)
            away2(n)
            own = part(n, 3) + hbuf[:, pl.ds(pl.multiple_of(n * CH, CH), CH)].astype(F32)
            @pl.when(n < nc - 1)
            def _():
                xsend(n).start()

            @pl.when(n == nc - 1)
            def _():
                xlast(0).start()
                xlast(1).start()
            osend(n).wait_recv()
            base[n] = base[n] + own
            for k, at in enumerate(EARLY):
                @pl.when(n == at)
                def _():
                    service(k)
            return 0

        lax.fori_loop(1, nc, step, 0)
        for n in (nc - 2, nc - 1):
            rsend(n).wait_send()
            osend(n).wait_send()

    pl.run_scoped(produce,
                  pltpu.VMEM((4, 3 * ln, ns), BF16),
                  pltpu.VMEM((2, 4, el, capd, CH), BF16),
                  pltpu.VMEM((2, 2, ln, CH), F32),
                  pltpu.VMEM((ln, d), BF16))

    def main(acc, wbuf, abuf0, abuf1):
        def wcopy(n, i):
            src = hbms[i // wj].at[pl.ds(pl.multiple_of(n * CH, CH), CH), pl.ds((i % wj) * WN, WN)]
            return pltpu.make_async_copy(src, wbuf.at[i % NS], s_w.at[i % NS])

        def ocopy(g, i):
            wd = min(WN, d - i * WN)
            src = wo_hbm.at[pl.ds(pl.multiple_of(g * CH, CH), CH), pl.ds(i * WN, wd)]
            return pltpu.make_async_copy(src, wbuf.at[i, :, 0:wd], s_w.at[i])

        for i in range(NS):
            wcopy(0, i).start()

        ssq[...] = jnp.zeros_like(ssq)

        def clear(n):
            xsend(n).wait_send()
            send[n] = jnp.zeros(send.shape[1:], F32)

        nj = 3 * wj

        def chunk(n, first):
            @pl.when((n + 1 >= len(EARLY)) & (n + 1 < nc - 1))
            def _():
                service(n + 1)

            @pl.when(n == nc - 2)
            def _():
                service_last(0)
            @pl.when(n >= 2)
            def _():
                clear(n - 2)
            @pl.when(n < nc - 1)
            def _():
                ysend(n).wait_recv()

            @pl.when(n == nc - 1)
            def _():
                ylast(0).wait_recv()
                ylast(1).wait_recv()
            yf = yin[n].astype(F32)
            y2 = yf * yf
            ssq[...] += y2[:, 0:128] + y2[:, 128:256] + y2[:, 256:384] + y2[:, 384:512]
            xw = (yf * (nw_ref[n] * SHIFT)).astype(BF16)
            for i in range(nj):
                if i == LATE:
                    @pl.when(n == nc - 2)
                    def _():
                        service_last(1)
                wcopy(n, i).wait()
                for b in range(WN // CH):
                    k = i * (WN // CH) + b
                    r = jnp.dot(xw, wbuf[i % NS, :, b * CH:(b + 1) * CH], preferred_element_type=F32)
                    acc[k] = r if first else acc[k] + r
                if i + NS < nj:
                    wcopy(n, i + NS).start()
                else:
                    ii = i + NS - nj

                    @pl.when(n + 1 < nc)
                    def _():
                        wcopy(n + 1, ii).start()

                    @pl.when(n + 1 == nc)
                    def _():
                        ocopy(0, ii).start()

        def later(n, _):
            chunk(n, False)
            return 0

        chunk(0, True)
        lax.fori_loop(1, nc, later, 0)
        ysend(nc - 2).wait_send()
        ylast(0).wait_send()
        ylast(1).wait_send()
        clear(nc - 2)
        xlast(0).wait_send()
        xlast(1).wait_send()
        send[nc - 1] = jnp.zeros(send.shape[1:], F32)
        ms = jnp.sum(ssq[...], axis=1, keepdims=True) / d
        rs_ref[...] = jnp.broadcast_to(lax.rsqrt(ms + EPS) * (1.0 / SHIFT), rs_ref.shape)

        tri = lax.broadcasted_iota(jnp.int32, (QB, QB), 0) >= lax.broadcasted_iota(jnp.int32, (QB, QB), 1)

        def qkv(g, hh):
            rs = rs_ref[:, 0:1]
            c = slice(hh * HEAD, (hh + 1) * HEAD)
            return [(acc[m * ng + g, :, c] * rs).astype(BF16) for m in range(3)]

        def heads(g, hhs, dst):
            tiles = [(hh, r) for hh in hhs for r in range(ln // QB)]
            qk = {hh: qkv(g, hh) for hh in hhs}
            sc = []
            for hh, r in tiles:
                lo, hi = r * QB, (r + 1) * QB
                q, k, _ = qk[hh]
                s = lax.dot_general(q[lo:hi], k[0:hi], (((1,), (1,)), ((), ())), preferred_element_type=F32)
                t = jnp.where(tri, s[:, lo:hi], MASKED)
                sc.append(t if r == 0 else jnp.concatenate([s[:, 0:lo], t], axis=1))
            mx = [jnp.max(s, axis=1, keepdims=True) for s in sc]
            ex = [jnp.exp2((s - m) * SCALE2) for s, m in zip(sc, mx)]
            rc = [1.0 / jnp.sum(e, axis=1, keepdims=True) for e in ex]
            pr = [(e * c).astype(BF16) for e, c in zip(ex, rc)]
            for (hh, r), w in zip(tiles, pr):
                lo, hi = r * QB, (r + 1) * QB
                dst[lo:hi, hh * HEAD:(hh + 1) * HEAD] = jnp.dot(w, qk[hh][2][0:hi], preferred_element_type=F32).astype(BF16)

        heads(0, range(CH // HEAD), abuf0)

        def group(g, src, dst):
            g1 = jnp.minimum(g + 1, ng - 1)
            for i in range(NS):
                ocopy(g, i).wait()
                wd = min(WN, d - i * WN)
                for b in range(wd // CH):
                    k = i * (WN // CH) + b
                    send[k] += jnp.dot(src[...], wbuf[i, :, b * CH:(b + 1) * CH], preferred_element_type=F32)
                if HEADS_AT[i]:
                    heads(g1, HEADS_AT[i], dst)

                @pl.when(g + 1 < ng)
                def _():
                    ocopy(g + 1, i).start()

        def pair(gg, _):
            group(2 * gg, abuf0, abuf1)
            group(2 * gg + 1, abuf1, abuf0)
            return 0

        lax.fori_loop(0, ng // 2, pair, 0)

        def fin(n, _):
            z_hbm[:, pl.ds(pl.multiple_of(n * CH, CH), CH)] = (
                yin[n].astype(F32) + send[n].astype(BF16).astype(F32)).astype(BF16)
            return 0
        lax.fori_loop(0, nc, fin, 0)

    pl.run_scoped(main,
                  pltpu.VMEM((3 * ng, ln, CH), F32),
                  pltpu.VMEM((NS, CH, WN), BF16),
                  pltpu.VMEM((ln, CH), BF16),
                  pltpu.VMEM((ln, CH), BF16))


def solution(mesh):
    n = mesh.shape['ep']
    sp_o = P('pp', 'data', 'ep', None, None)
    sp_r = P('pp', 'data', None, None, None)
    sp_1 = P('pp', None)
    sp_w = P('pp', None, None)

    def body(o, idx, slot, gate, h, norm_w, wq, wk, wv, wo):
        el, c, d = o.shape[2:]
        capd = c // n
        ln = h.shape[3]
        nc = d // CH
        ng = wq.shape[2] // CH
        sem = pltpu.SemaphoreType.DMA
        vm = pl.BlockSpec(memory_space=pltpu.VMEM)
        hb = pl.BlockSpec(memory_space=pltpu.HBM)
        z = pl.pallas_call(
            functools.partial(kernel, n, el, capd),
            out_shape=pltpu.VMEM((ln, d), BF16),
            in_specs=[vm] * 4 + [hb] * 6,
            out_specs=vm,
            scratch_shapes=[
                pltpu.VMEM((nc, ln, CH), F32),
                pltpu.VMEM((nc, ln, CH), F32),
                pltpu.VMEM((nc, ln, CH), F32),
                pltpu.VMEM((nc, ln, CH), BF16),
                pltpu.VMEM((ln, 128), F32),
                pltpu.VMEM((ln, 128), F32),
                pltpu.VMEM((2, ln, CH), BF16),
                sem((2,)), sem((nc,)), sem((2,)), sem((nc,)), sem((nc + 1,)), sem((nc + 1,)), sem((3,)), sem((nc + 1,)),
                sem((NS,)), sem((2, 4)), sem,
            ],
            compiler_params=pltpu.CompilerParams(collective_id=0, has_side_effects=True, vmem_limit_bytes=63000000),
        )(jnp.swapaxes(idx[0, 0], 1, 2), jnp.swapaxes(slot[0, 0], 1, 2), jnp.swapaxes(gate[0, 0], 1, 2), norm_w.reshape(nc, 1, CH), o.reshape(el, n, capd, d), h[0, 0, 0],
          wq[0], wk[0], wv[0], wo[0])
        return z.reshape(1, 1, 1, ln, d)

    return jax.shard_map(body, mesh=mesh, in_specs=(sp_o, sp_r, sp_r, sp_r, sp_o, sp_1, sp_w, sp_w, sp_w, sp_w), out_specs=sp_o, check_vma=False)
```
